32 devices in a mesh: member: 2 (over x), row: 16 (over z, y, core).
Axes of the slice: x: 2, y: 2, z: 4, core: 2. Of those that a mesh axis runs over, the one named last changes fastest.
Arguments:
- field: float32 [8, 6, 2048, 2048], P('member', None, 'row'), parts along dimension 0, as said below
- host: float32 [128, 2, 8, 6, 128], P('row', None, 'member'), parts along dimension 2, may hold values from -0.12 to 0.12
- weights: float32 [8, 4], replicated, may hold values from 0.1 to 1
- cut_x: int32 [6], replicated, may hold values from 16 to 63
- cut_y: int32 [6], replicated, may hold values from 16 to 63
- table_index: int32 [6], replicated, may hold values from 0 to 7
Outputs:
- nudged: float32 [8, 6, 2048, 2048], P('member', None, 'row'), parts along dimension 0
The draws below stay inside these ranges and needn't reach their ends.
There are 2 independent parts, one for each index of `member`. The reference program is written for one: setup_inputs(seed, part) draws one part's arguments, and reference() takes and returns one part's arrays. A program takes and returns all parts, laid end to end along the dimension named above; an argument that names none is the same for every part. Nothing has to cross between parts.
Inputs may be any that keep to these rules, and one draw needn't show every extreme that they name: `field`: real-valued fields with strong large-scale structure.
All inputs are finite; a program needn't handle non-finite values.
Results may differ from the reference program's by a relative error of at most 0.00005.
Values sent between devices are 32-bit elements; how exact they have to be, the bound alone decides.
A program may use at most 128 MiB of HBM per device.

```python
import math
import jax
import jax.numpy as jnp
from jax import lax

NX = 2048
NY = 2048
VARS = 4
LEVELS = 6
KHALF = 64
TABLE = 8
KBOX = 128


def draw_field(key, part):
    first_key, second_key = jax.random.split(jax.random.fold_in(key, 17), 2)
    signed = jnp.arange(KBOX, dtype=jnp.int32) - KHALF
    phase_x = jnp.mod(jnp.arange(NX, dtype=jnp.int32)[:, None] * signed[None, :], NX).astype(jnp.float32) * (2.0 * math.pi / NX)
    phase_y = jnp.mod(jnp.arange(NY, dtype=jnp.int32)[:, None] * signed[None, :], NY).astype(jnp.float32) * (2.0 * math.pi / NY)
    coeffs = 0.011 * jax.random.normal(second_key, (2, VARS, LEVELS, KBOX, KBOX), jnp.float32)
    noise = 0.5 * jax.random.normal(first_key, (VARS, LEVELS, NX, NY), jnp.float32)
    cos_x = jnp.cos(phase_x)
    sin_x = jnp.sin(phase_x)
    real_part = jnp.einsum('xa,vlab->vlxb', cos_x, coeffs[0]) - jnp.einsum('xa,vlab->vlxb', sin_x, coeffs[1])
    imag_part = jnp.einsum('xa,vlab->vlxb', sin_x, coeffs[0]) + jnp.einsum('xa,vlab->vlxb', cos_x, coeffs[1])
    smooth = jnp.einsum('vlxb,yb->vlxy', real_part, jnp.cos(phase_y)) - jnp.einsum('vlxb,yb->vlxy', imag_part, jnp.sin(phase_y))
    return (smooth + noise).astype(jnp.float32)


def set_ends(drawn, own_key, low, high):
    longest = drawn.shape.index(max(drawn.shape))
    spots = []
    for shift in (0, 1):
        where = [jax.random.randint(jax.random.fold_in(own_key, axis), (), 0, length) for axis, length in enumerate(drawn.shape)]
        where[longest] = (where[longest] + shift) % drawn.shape[longest]
        spots.append(tuple(where))
    return drawn.at[spots[0]].set(low).at[spots[1]].set(high)


def shard_levels(stream_key, shape, pieces, low, high):
    level = 1.0
    for position, blocks in pieces:
        draws = jax.random.uniform(jax.random.fold_in(jax.random.fold_in(stream_key, 6), position), (blocks,), jnp.float32, low / len(pieces), high / len(pieces))
        level = level * jnp.repeat(jnp.exp(draws), shape[position] // blocks).reshape((-1,) + (1,) * (len(shape) - 1 - position))
    return level


def centred(stream_key, extent, spread, limit, cuts=(), kind=jnp.bfloat16):
    values = jax.random.normal(stream_key, extent, jnp.float32) * spread
    if len(cuts) > 0:
        values = shard_levels(stream_key, extent, cuts, -0.22, 0.18) * values
    return jnp.clip(values, min=-limit, max=limit).astype(kind)


def setup_inputs(seed: int = 0, part: int = 0) -> dict:
    keys = jax.random.split(jax.random.key(seed), 7)
    part_splits = jax.random.split(jax.random.fold_in(keys[6], part), 7)
    field = draw_field(jax.random.fold_in(jax.random.fold_in(keys[6], part), 71), part)
    host = centred(part_splits[1], (KBOX, 2, VARS, LEVELS, KBOX), 0.02, 0.12, ((0, 16),), jnp.float32)
    weights = jnp.clip(jnp.exp(jax.random.uniform(keys[2], (TABLE, VARS), jnp.float32, math.log(0.1), math.log(1.0))), 0.1, 1.0)
    cut_x = set_ends(jax.random.randint(keys[3], (LEVELS,), KHALF // 4, KHALF), jax.random.fold_in(keys[3], 1), KHALF // 4, KHALF - 1).astype(jnp.int32)
    cut_y = set_ends(jax.random.randint(keys[4], (LEVELS,), KHALF // 4, KHALF), jax.random.fold_in(keys[4], 1), KHALF // 4, KHALF - 1).astype(jnp.int32)
    table_index = set_ends(jax.random.randint(keys[5], (LEVELS,), 0, TABLE), jax.random.fold_in(keys[5], 1), 0, TABLE - 1).astype(jnp.int32)
    return dict(field=field, host=host, weights=weights, cut_x=cut_x, cut_y=cut_y, table_index=table_index)


def box_wave(index):
    half = index // 2
    return jnp.where(index % 2 == 0, half, jnp.where(index == 1, -KHALF, -half)).astype(jnp.int32)


def reference(field, host, weights, cut_x, cut_y, table_index):
    signed = jnp.arange(KBOX, dtype=jnp.int32) - KHALF
    y_waves = box_wave(jnp.arange(KBOX, dtype=jnp.int32))
    onehot = (table_index[:, None] == jnp.arange(TABLE, dtype=jnp.int32)[None, :]).astype(jnp.float32)
    blend = jnp.dot(onehot, weights, precision=lax.Precision.HIGHEST)
    mask_x = (jnp.abs(signed)[None, :] <= cut_x[:, None]).astype(jnp.float32)
    mask_y = (jnp.abs(y_waves)[None, :] <= cut_y[:, None]).astype(jnp.float32)
    index_x = jnp.mod(signed, NX).astype(jnp.int32)
    index_y = jnp.mod(y_waves, NY).astype(jnp.int32)
    flat = field.reshape(VARS * LEVELS, NX, NY)

    def forward(grid):
        spectrum = jnp.fft.fft2(grid) / (NX * NY)
        boxed = spectrum[index_x[:, None], index_y[None, :]]
        return jnp.stack([jnp.real(boxed), jnp.imag(boxed)], 0).astype(field.dtype)

    boxes = lax.map(forward, flat).reshape(VARS, LEVELS, 2, KBOX, KBOX)
    spectrum = jnp.transpose(boxes, (4, 2, 0, 1, 3))
    scale = blend.T[None, None, :, :, None] * mask_y.T[:, None, None, :, None] * mask_x[None, None, None, :, :]
    delta = scale * (host - spectrum)
    ordered = jnp.transpose(delta, (2, 3, 1, 4, 0)).reshape(VARS * LEVELS, 2, KBOX, KBOX)

    def inverse(pair):
        grid, parts = pair
        boxed = parts[0] + 1j * parts[1]
        whole = jnp.zeros((NX, NY), dtype=boxed.dtype)
        whole = whole.at[index_x[:, None], index_y[None, :]].set(boxed)
        correction = jnp.real(jnp.fft.ifft2(whole)) * (NX * NY)
        return grid + correction.astype(grid.dtype)

    result = lax.map(inverse, (flat, ordered))
    return result.reshape(VARS, LEVELS, NX, NY)
```

```python
import functools
import math

import jax
import jax.numpy as jnp
import numpy as np
from jax import lax
from jax.experimental import pallas as pl
from jax.experimental.pallas import tpu as pltpu
from jax.sharding import PartitionSpec as P

TABLE = 8
MESH = pl.DeviceIdType.MESH
HIGHEST = lax.Precision.HIGHEST


def box_wave(index, khalf):
    half = index // 2
    return jnp.where(index % 2 == 0, half, jnp.where(index == 1, -khalf, -half))


def wave_tables(positions, length, waves):
    phase = jnp.mod(positions[:, None] * waves[None, :], length).astype(jnp.float32) * (
        2.0 * math.pi / length
    )
    return (jnp.cos(phase), jnp.sin(phase))


def scales(weights, cut_x, cut_y, table_index, x_waves, own_waves):
    onehot = (table_index[:, None] == lax.iota(jnp.int32, TABLE)[None, :]).astype(jnp.float32)
    blend = jnp.dot(onehot, weights, precision=HIGHEST)
    mask_x = (jnp.abs(x_waves)[None, :] <= cut_x[:, None]).astype(jnp.float32)
    mask_y = (jnp.abs(own_waves)[:, None] <= cut_y[None, :]).astype(jnp.float32)
    return (
        blend.T[None, :, :, None] * mask_y[:, None, :, None] * mask_x[None, None, :, :]
    )


def general(field, host, weights, cut_x, cut_y, table_index):
    row_count, ny = field.shape[2:]
    owned, kbox = host.shape[0], host.shape[-1]
    devices = lax.axis_size("row")
    nx = row_count * devices
    place = lax.axis_index("row")
    local_rows = place * row_count + lax.iota(jnp.int32, row_count)
    x_waves = lax.iota(jnp.int32, kbox) - kbox // 2
    y_waves = box_wave(lax.iota(jnp.int32, kbox), kbox // 2)
    cos_y, sin_y = wave_tables(lax.iota(jnp.int32, ny), ny, y_waves)
    table_y = jnp.stack([cos_y, -sin_y], 1) / ny
    spread = jnp.einsum("vlxy,yck->kcvlx", field, table_y, precision=HIGHEST)
    cosine, sine = wave_tables(local_rows, nx, x_waves)
    moved = lax.all_to_all(spread, "row", split_axis=0, concat_axis=4, tiled=True)
    cos_all, sin_all = wave_tables(lax.iota(jnp.int32, nx), nx, x_waves)
    cos_all, sin_all = cos_all / nx, sin_all / nx
    table = jnp.stack([jnp.stack([cos_all, -sin_all], 1), jnp.stack([sin_all, cos_all], 1)], 0)
    spectrum = jnp.einsum("kcvlx,cxdq->kdvlq", moved, table, precision=HIGHEST)
    own_waves = box_wave(place * owned + lax.iota(jnp.int32, owned), kbox // 2)
    scale = scales(weights, cut_x, cut_y, table_index, x_waves, own_waves)
    delta = scale[:, None] * (host - spectrum)
    slab = lax.all_gather(delta, "row", axis=0, tiled=True)
    table = jnp.stack([jnp.stack([cosine.T, sine.T], 1), jnp.stack([-sine.T, cosine.T], 1)], 0)
    back = jnp.einsum("kcvlq,cqdx->kdvlx", slab, table, precision=HIGHEST)
    table_back = jnp.stack([cos_y.T, -sin_y.T], 1)
    return field + jnp.einsum("kcvlx,kcy->vlxy", back, table_back, precision=HIGHEST)


def halves(values):
    high = values.astype(jnp.bfloat16)
    return high, (values - high.astype(jnp.float32)).astype(jnp.bfloat16)


def np_halves(values):
    values = values.astype(np.float32)
    high = values.astype(jnp.bfloat16)
    return high, (values - high.astype(np.float32)).astype(jnp.bfloat16)


def real_modes(length, waves, is_sine):
    phase = (np.arange(length)[:, None] * waves[None, :]) % length * (2.0 * np.pi / length)
    return np.where(is_sine[None, :], np.sin(phase), np.cos(phase))


def forward_kernel(rows, field_ref, table_ref, x_ref, out_ref):
    _, count, row_count, ny = field_ref.shape
    kbox = x_ref.shape[1]
    high, low = halves(field_ref[...].reshape(count * row_count, ny))
    both = jnp.dot(high, table_ref[...], preferred_element_type=jnp.float32)
    rest = jnp.dot(low, table_ref[:, :kbox], preferred_element_type=jnp.float32)
    part = both[:, :kbox] + both[:, kbox:] + rest
    for k in range(count):
        moded = lax.dot_general(
            part[k * row_count : (k + 1) * row_count],
            x_ref[...],
            (((0,), (0,)), ((), ())),
            precision=HIGHEST,
            preferred_element_type=jnp.float32,
        )
        out_ref[:, k] = moded.reshape(out_ref.shape[0], rows, kbox)


def inverse_kernel(field_ref, modes_ref, table_ref, x_ref, out_ref):
    _, count, row_count, ny = field_ref.shape
    kbox = x_ref.shape[1]
    parts = [
        lax.dot_general(
            x_ref[...],
            modes_ref[:, k].reshape(kbox, kbox),
            (((1,), (1,)), ((), ())),
            precision=HIGHEST,
            preferred_element_type=jnp.float32,
        )
        for k in range(count)
    ]
    high, low = halves(jnp.concatenate(parts, 0))
    added = jnp.dot(
        jnp.concatenate([high, high], 1), table_ref[...], preferred_element_type=jnp.float32
    )
    added += jnp.dot(low, table_ref[:kbox], preferred_element_type=jnp.float32)
    out_ref[...] = field_ref[...] + added.reshape(field_ref.shape)


def exchange_kernel(
    bits, orders, owned, norm, part_ref, host_ref, scale_ref, mc_ref, ms_ref, out_ref, *scratch
):
    pipes = len(orders)
    got = [scratch[q * bits : (q + 1) * bits] for q in range(pipes)]
    kept = [scratch[(pipes + q) * bits : (pipes + q + 1) * bits] for q in range(pipes)]
    send_sem, recv_sem = scratch[2 * pipes * bits :]
    me = lax.axis_index("row")
    member = lax.axis_index("member")
    mine = [(me // (1 << b)) % 2 for b in range(bits)]
    peer = [me + (1 << b) * (1 - 2 * mine[b]) for b in range(bits)]
    rows = part_ref.shape[-2]
    span = rows // pipes

    barrier = pltpu.get_barrier_semaphore()
    for b in range(bits):
        pl.semaphore_signal(barrier, inc=1, device_id=(member, peer[b]), device_id_type=MESH)
    pl.semaphore_wait(barrier, bits)

    def pick(ref, order, step, flip):
        left = sorted(order[step:], reverse=True)
        bit = order[step]
        index = tuple(
            (1 - mine[bit] if flip else mine[bit]) if b == bit else slice(None) for b in left
        )
        return index

    def reduce_copy(q, step):
        order = orders[q]
        index = pick(None, order, step, True)
        if step == 0:
            source = part_ref.at[index + (pl.ds(q * span, span),)]
        else:
            source = kept[q][step - 1].at[index]
        return pltpu.make_async_remote_copy(
            src_ref=source,
            dst_ref=got[q][step],
            send_sem=send_sem.at[q, step],
            recv_sem=recv_sem.at[q, step],
            device_id=(member, peer[order[step]]),
            device_id_type=MESH,
        )

    copies = [reduce_copy(q, 0) for q in range(pipes)]
    for copy in copies:
        copy.start()
    for step in range(bits):
        for q in range(pipes):
            copies[q].wait()
            index = pick(None, orders[q], step, False)
            if step == 0:
                own = part_ref[index + (pl.ds(q * span, span),)]
            else:
                own = kept[q][step - 1][index]
            kept[q][step][...] = own + got[q][step][...]
            if step + 1 < bits:
                copies[q] = reduce_copy(q, step + 1)
                copies[q].start()

    half = owned // 2
    line = lax.broadcasted_iota(jnp.int32, (span, 1), 0) % owned < half

    def swap(values):
        return jnp.where(
            line, pltpu.roll(values, span - half, 0), pltpu.roll(values, half, 0)
        )

    def mix(values, ref, axis):
        return lax.dot_general(
            values,
            ref[...],
            (((1,), (axis,)), ((), ())),
            precision=HIGHEST,
            preferred_element_type=jnp.float32,
        )

    def gather_copy(q, step):
        order = orders[q]
        fixed = order[: step + 1]
        index = tuple(mine[b] if b in fixed else slice(None) for b in range(bits - 1, -1, -1))
        block = out_ref.at[index + (pl.ds(q * span, span),)]
        return pltpu.make_async_remote_copy(
            src_ref=block,
            dst_ref=block,
            send_sem=send_sem.at[q, bits + step],
            recv_sem=recv_sem.at[q, bits + step],
            device_id=(member, peer[order[step]]),
            device_id_type=MESH,
        )

    own_index = tuple(mine[b] for b in range(bits - 1, -1, -1))
    for q in range(pipes):
        total = kept[q][bits - 1][...] * norm
        even, odd = mix(total, mc_ref, 0), mix(total, ms_ref, 0)
        even_s, odd_s = swap(even), swap(odd)
        real = jnp.where(line, even - odd_s, even_s + odd)
        imag = jnp.where(line, -(odd + even_s), even - odd_s)
        here = pl.ds(q * span, span)
        real = scale_ref[here] * (host_ref[0, here] - real)
        imag = scale_ref[here] * (host_ref[1, here] - imag)
        real_s, imag_s = swap(real), swap(imag)
        cosine = jnp.where(line, real + real_s, imag - imag_s)
        sine = jnp.where(line, -(imag + imag_s), real - real_s)
        out_ref[own_index + (here,)] = mix(cosine, mc_ref, 1) + mix(sine, ms_ref, 1)
        copies[q] = gather_copy(q, bits - 1)
        copies[q].start()
    for step in range(bits - 1, -1, -1):
        for q in range(pipes):
            copies[q].wait()
            if step > 0:
                copies[q] = gather_copy(q, step - 1)
                copies[q].start()


def exchange(part, host, scale, mc, ms, devices, owned, norm):
    bits = devices.bit_length() - 1
    rows, kbox = part.shape[-2:]
    cube = (2,) * bits
    plain = list(range(bits))
    orders = [plain, [0] + plain[2:] + [1]]
    pipes = len(orders)
    sizes = [
        pltpu.VMEM((2,) * (bits - 1 - step) + (rows // pipes, kbox), jnp.float32)
        for step in range(bits)
    ]
    vmem = pl.BlockSpec(memory_space=pltpu.VMEM)
    out = pl.pallas_call(
        functools.partial(exchange_kernel, bits, orders, owned, norm),
        out_shape=jax.ShapeDtypeStruct(cube + (rows, kbox), jnp.float32),
        in_specs=[vmem] * 5,
        out_specs=vmem,
        scratch_shapes=sizes * (2 * pipes)
        + [pltpu.SemaphoreType.DMA((pipes, 2 * bits)), pltpu.SemaphoreType.DMA((pipes, 2 * bits))],
        compiler_params=pltpu.CompilerParams(
            collective_id=0, has_side_effects=True, vmem_limit_bytes=32 * 1024 * 1024
        ),
    )(part.reshape(cube + (rows, kbox)), host, scale, mc, ms)
    return out


def nudge(field, host, weights, cut_x, cut_y, table_index):
    variables, levels, row_count, ny = field.shape
    owned, kbox = host.shape[0], host.shape[-1]
    khalf, half = kbox // 2, owned // 2
    devices = lax.axis_size("row")
    nx = row_count * devices
    place = lax.axis_index("row")
    fields = variables * levels

    column = np.arange(kbox)
    y_wave = column // owned * half + column % half
    y_sine = column % owned >= half
    y_high, y_low = np_halves(real_modes(ny, y_wave, y_sine))
    table_y = jnp.asarray(np.concatenate([y_high, y_low], 1))
    table_back = jnp.asarray(np.concatenate([y_high.T, y_low.T], 0))
    x_all = real_modes(nx, column % khalf, column >= khalf).astype(np.float32)
    table_x = lax.dynamic_slice_in_dim(jnp.asarray(x_all), place * row_count, row_count, 0)
    wave = column - khalf
    inside = np.abs(wave) < khalf
    mc = ((column[:, None] == np.abs(wave)[None, :]) & inside).astype(np.float32)
    ms = ((column[:, None] == np.abs(wave)[None, :] + khalf) & inside) * np.sign(wave)
    ms = ms.astype(np.float32)

    group = math.gcd(levels, 3)
    steps = levels // group
    grid_block = pl.BlockSpec((1, group, row_count, ny), lambda v, g: (v, g, 0, 0))
    mode_block = pl.BlockSpec(
        (devices, group, owned, kbox), lambda v, g: (0, v * steps + g, 0, 0)
    )

    def whole(*shape):
        return pl.BlockSpec(shape, lambda v, g: (0,) * len(shape))

    params = pltpu.CompilerParams(vmem_limit_bytes=48 * 1024 * 1024)
    part = pl.pallas_call(
        functools.partial(forward_kernel, owned),
        grid=(variables, steps),
        out_shape=jax.ShapeDtypeStruct((devices, fields, owned, kbox), jnp.float32),
        in_specs=[grid_block, whole(ny, 2 * kbox), whole(row_count, kbox)],
        out_specs=mode_block,
        compiler_params=params,
    )(field, table_y, table_x)

    row = place * owned + lax.iota(jnp.int32, owned)
    own_waves = box_wave(row, khalf)
    scale = scales(weights, cut_x, cut_y, table_index, lax.iota(jnp.int32, kbox) - khalf, own_waves)
    scale = scale.reshape(half, 2, fields, kbox).transpose(2, 1, 0, 3)
    placed = host.reshape(half, 2, 2, fields, kbox).transpose(2, 3, 1, 0, 4)
    modes = exchange(
        part.reshape(devices, fields * owned, kbox),
        placed.reshape(2, fields * owned, kbox),
        scale.reshape(fields * owned, kbox),
        jnp.asarray(mc),
        jnp.asarray(ms),
        devices,
        owned,
        1.0 / (nx * ny),
    ).reshape(devices, fields, owned, kbox)

    return pl.pallas_call(
        inverse_kernel,
        grid=(variables, steps),
        out_shape=jax.ShapeDtypeStruct(field.shape, jnp.float32),
        in_specs=[grid_block, mode_block, whole(2 * kbox, ny), whole(row_count, kbox)],
        out_specs=grid_block,
        compiler_params=params,
    )(field, modes, table_back, table_x)


def shards(*args):
    khalf = args[1].shape[-1] // 2
    cut_x, cut_y = args[3:5]
    edge = jnp.maximum(jnp.max(cut_x), jnp.max(cut_y)) >= khalf
    return lax.cond(edge, general, nudge, *args)


def solution(mesh):
    return jax.shard_map(
        shards,
        mesh=mesh,
        in_specs=(
            P("member", None, "row", None),
            P("row", None, "member", None, None),
            P(),
            P(),
            P(),
            P(),
        ),
        out_specs=P("member", None, "row", None),
        check_vma=False,
    )
```

```python
import functools
import math

import jax
import jax.numpy as jnp
import numpy as np
from jax import lax
from jax.experimental import pallas as pl
from jax.experimental.pallas import tpu as pltpu
from jax.sharding import PartitionSpec as P

TABLE = 8
MESH = pl.DeviceIdType.MESH
HIGHEST = lax.Precision.HIGHEST


def box_wave(index, khalf):
    half = index // 2
    return jnp.where(index % 2 == 0, half, jnp.where(index == 1, -khalf, -half))


def wave_tables(positions, length, waves):
    phase = jnp.mod(positions[:, None] * waves[None, :], length).astype(jnp.float32) * (
        2.0 * math.pi / length
    )
    return (jnp.cos(phase), jnp.sin(phase))


def general(field, host, weights, cut_x, cut_y, table_index):
    variables, levels, row_count, ny = field.shape
    owned, kbox = host.shape[0], host.shape[-1]
    fields = variables * levels
    devices = lax.axis_size("row")
    nx = row_count * devices
    place = lax.axis_index("row")
    local_rows = place * row_count + lax.iota(jnp.int32, row_count)
    x_waves = lax.iota(jnp.int32, kbox) - kbox // 2
    y_waves = box_wave(lax.iota(jnp.int32, kbox), kbox // 2)
    own_waves = box_wave(place * owned + lax.iota(jnp.int32, owned), kbox // 2)
    onehot = (table_index[:, None] == lax.iota(jnp.int32, TABLE)[None, :]).astype(jnp.float32)
    blend = jnp.dot(onehot, weights, precision=HIGHEST)
    mask_x = (jnp.abs(x_waves)[None, :] <= cut_x[:, None]).astype(jnp.float32)
    mask_y = (jnp.abs(own_waves)[None, :] <= cut_y[:, None]).astype(jnp.float32)
    scale = blend.T[:, :, None, None] * mask_y[None, :, :, None] * mask_x[None, :, None, :]
    cos_y, sin_y = wave_tables(lax.iota(jnp.int32, ny), ny, y_waves)
    cos_x, sin_x = wave_tables(local_rows, nx, x_waves)
    table_y = jnp.concatenate([cos_y, -sin_y], 1)
    table_x = jnp.stack([jnp.concatenate([cos_x, -sin_x], 1), jnp.concatenate([sin_x, cos_x], 1)])

    def one(pair):
        grid, wanted, factor = pair
        spread = jnp.dot(grid, table_y, precision=HIGHEST).reshape(row_count, 2, kbox)
        parts = jnp.einsum("xck,cxq->kq", spread, table_x, precision=HIGHEST)
        parts = parts.reshape(devices, owned, 2, kbox)
        moved = lax.all_to_all(parts, "row", split_axis=0, concat_axis=0, tiled=True)
        spectrum = jnp.sum(moved, 0) / (nx * ny)
        delta = factor[:, None, :] * (wanted - spectrum)
        box = lax.all_gather(delta, "row", axis=0, tiled=True).reshape(kbox, 2 * kbox)
        back = jnp.einsum("kq,cxq->xck", box, table_x, precision=HIGHEST)
        return grid + jnp.dot(back.reshape(row_count, 2 * kbox), table_y.T, precision=HIGHEST)

    wanted = host.transpose(2, 3, 0, 1, 4).reshape(fields, owned, 2, kbox)
    result = lax.map(
        one, (field.reshape(fields, row_count, ny), wanted, scale.reshape(fields, owned, kbox))
    )
    return result.reshape(field.shape)


def halves(values):
    high = values.astype(jnp.bfloat16)
    return high, (values - high.astype(jnp.float32)).astype(jnp.bfloat16)


def np_halves(values):
    values = values.astype(np.float32)
    high = values.astype(jnp.bfloat16)
    return high, (values - high.astype(np.float32)).astype(jnp.bfloat16)


def real_modes(positions, length, waves, is_sine):
    if isinstance(positions, int):
        positions = np.arange(positions)
    phase = (positions[:, None] * waves[None, :]) % length * (2.0 * np.pi / length)
    return np.where(is_sine[None, :], np.sin(phase), np.cos(phase))


def local_modes(base_ref, turn_ref):
    count = base_ref.shape[0] // 2
    return base_ref[:count] * turn_ref[0, :1] + base_ref[count:] * turn_ref[0, 1:2]


def forward_kernel(owned, cut_x_ref, cut_y_ref, field_ref, table_ref, base_ref, turn_ref, out_ref, edge_ref):
    _, count, row_count, ny = field_ref.shape
    kbox = base_ref.shape[1]
    edge = cut_x_ref[0]
    for level in range(cut_x_ref.shape[0]):
        edge = jnp.maximum(edge, jnp.maximum(cut_x_ref[level], cut_y_ref[level]))
    edge_ref[0] = edge
    high, low = halves(field_ref[...].reshape(count * row_count, ny))
    both = jnp.dot(high, table_ref[...], preferred_element_type=jnp.float32)
    rest = jnp.dot(low, table_ref[:, :kbox], preferred_element_type=jnp.float32)
    part = both[:, :kbox] + both[:, kbox:] + rest
    x_high, x_low = halves(local_modes(base_ref, turn_ref))
    x_three = jnp.concatenate([x_high, x_high, x_low], 0)
    for k in range(count):
        high, low = halves(part[k * row_count : (k + 1) * row_count])
        moded = lax.dot_general(
            jnp.concatenate([high, low, high], 0),
            x_three,
            (((0,), (0,)), ((), ())),
            preferred_element_type=jnp.float32,
        )
        out_ref[:, k] = moded.reshape(out_ref.shape[0], owned, kbox)


def inverse_kernel(field_ref, modes_ref, table_ref, base_ref, turn_ref, out_ref, three_ref):
    _, count, row_count, ny = field_ref.shape
    kbox = base_ref.shape[1]
    x_high, x_low = halves(local_modes(base_ref, turn_ref))
    x_three = jnp.concatenate([x_high, x_high, x_low], 1)

    @pl.when((pl.program_id(0) == 0) & (pl.program_id(1) == 0))
    def _():
        three_ref[:kbox] = table_ref[:kbox]
        three_ref[kbox:] = table_ref[...]

    parts = []
    for k in range(count):
        high, low = halves(modes_ref[:, k].reshape(kbox, kbox))
        parts.append(
            lax.dot_general(
                x_three,
                jnp.concatenate([high, low, high], 1),
                (((1,), (1,)), ((), ())),
                preferred_element_type=jnp.float32,
            )
        )
    high, low = halves(jnp.concatenate(parts, 0))
    added = jnp.dot(
        jnp.concatenate([high, low, high], 1), three_ref[...], preferred_element_type=jnp.float32
    )
    out_ref[...] = field_ref[...] + added.reshape(field_ref.shape)


def exchange_kernel(
    bits, orders, owned, norm, weights_ref, cut_x_ref, cut_y_ref, index_ref,
    part_ref, host_ref, mc_ref, ms_ref, out_ref, *scratch
):
    pipes = len(orders)
    got = [scratch[q * bits : (q + 1) * bits] for q in range(pipes)]
    kept = [scratch[(pipes + q) * bits : (pipes + q + 1) * bits] for q in range(pipes)]
    scale_ref, send_sem, recv_sem = scratch[2 * pipes * bits :]
    me = lax.axis_index("row")
    member = lax.axis_index("member")
    mine = [(me // (1 << b)) % 2 for b in range(bits)]
    peer = [me + (1 << b) * (1 - 2 * mine[b]) for b in range(bits)]
    rows = part_ref.shape[-2]
    span = rows // pipes

    barrier = pltpu.get_barrier_semaphore()
    for b in range(bits):
        pl.semaphore_signal(barrier, inc=1, device_id=(member, peer[b]), device_id_type=MESH)
    pl.semaphore_wait(barrier, bits)

    def pick(ref, order, step, flip):
        left = sorted(order[step:], reverse=True)
        bit = order[step]
        index = tuple(
            (1 - mine[bit] if flip else mine[bit]) if b == bit else slice(None) for b in left
        )
        return index

    def reduce_copy(q, step):
        order = orders[q]
        index = pick(None, order, step, True)
        if step == 0:
            source = part_ref.at[index + (pl.ds(q * span, span),)]
        else:
            source = kept[q][step - 1].at[index]
        return pltpu.make_async_remote_copy(
            src_ref=source,
            dst_ref=got[q][step],
            send_sem=send_sem.at[q, step],
            recv_sem=recv_sem.at[q, step],
            device_id=(member, peer[order[step]]),
            device_id_type=MESH,
        )

    copies = [reduce_copy(q, 0) for q in range(pipes)]
    for copy in copies:
        copy.start()

    kbox = part_ref.shape[-1]
    half, khalf = owned // 2, kbox // 2
    row = lax.broadcasted_iota(jnp.int32, (rows, kbox), 0)
    column = lax.broadcasted_iota(jnp.int32, (rows, kbox), 1)
    line_of, slot = row // owned, row % owned
    wave = me * half + slot % half
    wave = jnp.where((wave == 0) & (slot >= half), khalf, wave)
    levels = cut_x_ref.shape[0]
    scale = jnp.zeros((rows, kbox), jnp.float32)
    for level in range(levels):
        kept_wave = (jnp.abs(column - khalf) <= cut_x_ref[level]) & (wave <= cut_y_ref[level])
        for v in range(rows // owned // levels):
            blend = jnp.where(kept_wave, weights_ref[index_ref[level], v], 0.0)
            scale = jnp.where(line_of == v * levels + level, blend, scale)
    scale_ref[...] = scale

    for step in range(bits):
        for q in range(pipes):
            copies[q].wait()
            index = pick(None, orders[q], step, False)
            if step == 0:
                own = part_ref[index + (pl.ds(q * span, span),)]
            else:
                own = kept[q][step - 1][index]
            kept[q][step][...] = own + got[q][step][...]
            if step + 1 < bits:
                copies[q] = reduce_copy(q, step + 1)
                copies[q].start()

    line = lax.broadcasted_iota(jnp.int32, (span, 1), 0) % owned < half

    def swap(values):
        return jnp.where(
            line, pltpu.roll(values, span - half, 0), pltpu.roll(values, half, 0)
        )

    def mix(values, ref, axis):
        return lax.dot_general(
            values,
            ref[...],
            (((1,), (axis,)), ((), ())),
            precision=HIGHEST,
            preferred_element_type=jnp.float32,
        )

    def gather_copy(q, step):
        order = orders[q]
        fixed = order[: step + 1]
        index = tuple(mine[b] if b in fixed else slice(None) for b in range(bits - 1, -1, -1))
        block = out_ref.at[index + (pl.ds(q * span, span),)]
        return pltpu.make_async_remote_copy(
            src_ref=block,
            dst_ref=block,
            send_sem=send_sem.at[q, bits + step],
            recv_sem=recv_sem.at[q, bits + step],
            device_id=(member, peer[order[step]]),
            device_id_type=MESH,
        )

    own_index = tuple(mine[b] for b in range(bits - 1, -1, -1))
    for q in range(pipes):
        total = kept[q][bits - 1][...] * norm
        even, odd = mix(total, mc_ref, 0), mix(total, ms_ref, 0)
        even_s, odd_s = swap(even), swap(odd)
        real = jnp.where(line, even - odd_s, even_s + odd)
        imag = jnp.where(line, -(odd + even_s), even - odd_s)
        here = pl.ds(q * span, span)
        real = scale_ref[here] * (host_ref[0, here] - real)
        imag = scale_ref[here] * (host_ref[1, here] - imag)
        real_s, imag_s = swap(real), swap(imag)
        cosine = jnp.where(line, real + real_s, imag - imag_s)
        sine = jnp.where(line, -(imag + imag_s), real - real_s)
        out_ref[own_index + (here,)] = mix(cosine, mc_ref, 1) + mix(sine, ms_ref, 1)
        copies[q] = gather_copy(q, bits - 1)
        copies[q].start()
    for step in range(bits - 1, -1, -1):
        for q in range(pipes):
            copies[q].wait()
            if step > 0:
                copies[q] = gather_copy(q, step - 1)
                copies[q].start()


def exchange(scalars, part, host, mc, ms, devices, owned, norm):
    bits = devices.bit_length() - 1
    rows, kbox = part.shape[-2:]
    cube = (2,) * bits
    plain = list(range(bits))
    orders = [plain, [0] + plain[2:] + [1]]
    pipes = len(orders)
    sizes = [
        pltpu.VMEM((2,) * (bits - 1 - step) + (rows // pipes, kbox), jnp.float32)
        for step in range(bits)
    ]
    vmem = pl.BlockSpec(memory_space=pltpu.VMEM)
    out = pl.pallas_call(
        functools.partial(exchange_kernel, bits, orders, owned, norm),
        out_shape=jax.ShapeDtypeStruct(cube + (rows, kbox), jnp.float32),
        in_specs=[pl.BlockSpec(memory_space=pltpu.SMEM)] * 4 + [vmem] * 4,
        out_specs=vmem,
        scratch_shapes=sizes * (2 * pipes)
        + [pltpu.VMEM((rows, kbox), jnp.float32)]
        + [pltpu.SemaphoreType.DMA((pipes, 2 * bits)), pltpu.SemaphoreType.DMA((pipes, 2 * bits))],
        compiler_params=pltpu.CompilerParams(
            collective_id=0, has_side_effects=True, vmem_limit_bytes=32 * 1024 * 1024
        ),
    )(*scalars, part.reshape(cube + (rows, kbox)), host, mc, ms)
    return out


def nudge(field, host, weights, cut_x, cut_y, table_index):
    variables, levels, row_count, ny = field.shape
    owned, kbox = host.shape[0], host.shape[-1]
    khalf, half = kbox // 2, owned // 2
    devices = lax.axis_size("row")
    nx = row_count * devices
    fields = variables * levels

    column = np.arange(kbox)
    y_wave = column // owned * half + column % half
    y_sine = column % owned >= half
    y_high, y_low = np_halves(real_modes(ny, ny, y_wave, y_sine))
    table_y = jnp.asarray(np.concatenate([y_high, y_low], 1))
    table_back = jnp.asarray(np.concatenate([y_high.T, y_low.T], 0))
    x_wave, x_sine = column % khalf, column >= khalf
    start = np.arange(devices) * row_count
    base = np.concatenate(
        [real_modes(row_count, nx, x_wave, column < 0), real_modes(row_count, nx, x_wave, column >= 0)]
    )
    turn_cos = real_modes(start, nx, x_wave, column < 0)
    turn_sin = real_modes(start, nx, x_wave, column >= 0)
    turn = np.stack(
        [np.where(x_sine, turn_sin, turn_cos), np.where(x_sine, turn_cos, -turn_sin)], 1
    )
    base = jnp.asarray(base.astype(np.float32))
    turn = jnp.asarray(turn.astype(np.float32))
    wave = column - khalf
    inside = np.abs(wave) < khalf
    mc = ((column[:, None] == np.abs(wave)[None, :]) & inside).astype(np.float32)
    ms = ((column[:, None] == np.abs(wave)[None, :] + khalf) & inside) * np.sign(wave)
    ms = ms.astype(np.float32)

    group = math.gcd(levels, 3)
    steps = levels // group
    grid_block = pl.BlockSpec((1, group, row_count, ny), lambda v, g: (v, g, 0, 0))
    mode_block = pl.BlockSpec(
        (devices, group, owned, kbox), lambda v, g: (0, v * steps + g, 0, 0)
    )

    def whole(*shape):
        return pl.BlockSpec(shape, lambda v, g: (0,) * len(shape))

    local_turn = pl.BlockSpec((1, 2, kbox), lambda v, g: (lax.axis_index("row"), 0, 0))
    scalar = pl.BlockSpec(memory_space=pltpu.SMEM)
    params = pltpu.CompilerParams(vmem_limit_bytes=48 * 1024 * 1024)
    part, edge = pl.pallas_call(
        functools.partial(forward_kernel, owned),
        grid=(variables, steps),
        out_shape=(
            jax.ShapeDtypeStruct((devices, fields, owned, kbox), jnp.float32),
            jax.ShapeDtypeStruct((1,), jnp.int32),
        ),
        in_specs=[scalar, scalar, grid_block, whole(ny, 2 * kbox), whole(2 * row_count, kbox), local_turn],
        out_specs=(mode_block, scalar),
        compiler_params=params,
    )(cut_x, cut_y, field, table_y, base, turn)

    placed = host.reshape(half, 2, 2, fields, kbox).transpose(2, 3, 1, 0, 4)
    modes = exchange(
        (weights, cut_x, cut_y, table_index),
        part.reshape(devices, fields * owned, kbox),
        placed.reshape(2, fields * owned, kbox),
        jnp.asarray(mc),
        jnp.asarray(ms),
        devices,
        owned,
        1.0 / (nx * ny),
    ).reshape(devices, fields, owned, kbox)

    inverse = pl.pallas_call(
        inverse_kernel,
        grid=(variables, steps),
        out_shape=jax.ShapeDtypeStruct(field.shape, jnp.float32),
        in_specs=[grid_block, mode_block, whole(2 * kbox, ny), whole(2 * row_count, kbox), local_turn],
        out_specs=grid_block,
        scratch_shapes=[pltpu.VMEM((3 * kbox, ny), jnp.bfloat16)],
        compiler_params=params,
    )
    return lax.cond(
        edge[0] >= khalf,
        lambda *args: general(*args[:6]),
        lambda *args: inverse(args[0], *args[6:]),
        field, host, weights, cut_x, cut_y, table_index, modes, table_back, base, turn,
    )


def solution(mesh):
    return jax.shard_map(
        nudge,
        mesh=mesh,
        in_specs=(
            P("member", None, "row", None),
            P("row", None, "member", None, None),
            P(),
            P(),
            P(),
            P(),
        ),
        out_specs=P("member", None, "row", None),
        check_vma=False,
    )
```

```python
import functools
import math

import jax
import jax.numpy as jnp
import numpy as np
from jax import lax
from jax.experimental import pallas as pl
from jax.experimental.pallas import tpu as pltpu
from jax.sharding import PartitionSpec as P

TABLE = 8
MESH = pl.DeviceIdType.MESH
HIGHEST = lax.Precision.HIGHEST


def box_wave(index, khalf):
    half = index // 2
    return jnp.where(index % 2 == 0, half, jnp.where(index == 1, -khalf, -half))


def wave_tables(positions, length, waves):
    phase = jnp.mod(positions[:, None] * waves[None, :], length).astype(jnp.float32) * (
        2.0 * math.pi / length
    )
    return (jnp.cos(phase), jnp.sin(phase))


def general(field, host, weights, cut_x, cut_y, table_index):
    variables, levels, row_count, ny = field.shape
    owned, kbox = host.shape[0], host.shape[-1]
    fields = variables * levels
    devices = lax.axis_size("row")
    nx = row_count * devices
    place = lax.axis_index("row")
    local_rows = place * row_count + lax.iota(jnp.int32, row_count)
    x_waves = lax.iota(jnp.int32, kbox) - kbox // 2
    y_waves = box_wave(lax.iota(jnp.int32, kbox), kbox // 2)
    own_waves = box_wave(place * owned + lax.iota(jnp.int32, owned), kbox // 2)
    onehot = (table_index[:, None] == lax.iota(jnp.int32, TABLE)[None, :]).astype(jnp.float32)
    blend = jnp.dot(onehot, weights, precision=HIGHEST)
    mask_x = (jnp.abs(x_waves)[None, :] <= cut_x[:, None]).astype(jnp.float32)
    mask_y = (jnp.abs(own_waves)[None, :] <= cut_y[:, None]).astype(jnp.float32)
    scale = blend.T[:, :, None, None] * mask_y[None, :, :, None] * mask_x[None, :, None, :]
    cos_y, sin_y = wave_tables(lax.iota(jnp.int32, ny), ny, y_waves)
    cos_x, sin_x = wave_tables(local_rows, nx, x_waves)
    table_y = jnp.concatenate([cos_y, -sin_y], 1)
    table_x = jnp.stack([jnp.concatenate([cos_x, -sin_x], 1), jnp.concatenate([sin_x, cos_x], 1)])

    def one(pair):
        grid, wanted, factor = pair
        spread = jnp.dot(grid, table_y, precision=HIGHEST).reshape(row_count, 2, kbox)
        parts = jnp.einsum("xck,cxq->kq", spread, table_x, precision=HIGHEST)
        parts = parts.reshape(devices, owned, 2, kbox)
        moved = lax.all_to_all(parts, "row", split_axis=0, concat_axis=0, tiled=True)
        spectrum = jnp.sum(moved, 0) / (nx * ny)
        delta = factor[:, None, :] * (wanted - spectrum)
        box = lax.all_gather(delta, "row", axis=0, tiled=True).reshape(kbox, 2 * kbox)
        back = jnp.einsum("kq,cxq->xck", box, table_x, precision=HIGHEST)
        return grid + jnp.dot(back.reshape(row_count, 2 * kbox), table_y.T, precision=HIGHEST)

    wanted = host.transpose(2, 3, 0, 1, 4).reshape(fields, owned, 2, kbox)
    result = lax.map(
        one, (field.reshape(fields, row_count, ny), wanted, scale.reshape(fields, owned, kbox))
    )
    return result.reshape(field.shape)


def halves(values):
    high = values.astype(jnp.bfloat16)
    return high, (values - high.astype(jnp.float32)).astype(jnp.bfloat16)


def np_halves(values):
    values = values.astype(np.float32)
    high = values.astype(jnp.bfloat16)
    return high, (values - high.astype(np.float32)).astype(jnp.bfloat16)


def real_modes(positions, length, waves, is_sine):
    if isinstance(positions, int):
        positions = np.arange(positions)
    phase = (positions[:, None] * waves[None, :]) % length * (2.0 * np.pi / length)
    return np.where(is_sine[None, :], np.sin(phase), np.cos(phase))


def local_modes(base_ref, turn_ref):
    count = base_ref.shape[0] // 2
    return base_ref[:count] * turn_ref[0, :1] + base_ref[count:] * turn_ref[0, 1:2]


def inverse_kernel(field_ref, modes_ref, table_ref, base_ref, turn_ref, out_ref, three_ref):
    _, count, row_count, ny = field_ref.shape
    kbox = base_ref.shape[1]
    owned = modes_ref.shape[2] // count
    x_high, x_low = halves(local_modes(base_ref, turn_ref))
    x_three = jnp.concatenate([x_high, x_high, x_low], 1)

    @pl.when((pl.program_id(0) == 0) & (pl.program_id(1) == 0))
    def _():
        three_ref[:kbox] = table_ref[:kbox]
        three_ref[kbox:] = table_ref[...]

    parts = []
    for k in range(count):
        high, low = halves(modes_ref[0, :, k * owned : (k + 1) * owned].reshape(kbox, kbox))
        parts.append(
            lax.dot_general(
                x_three,
                jnp.concatenate([high, low, high], 1),
                (((1,), (1,)), ((), ())),
                preferred_element_type=jnp.float32,
            )
        )
    high, low = halves(jnp.concatenate(parts, 0))
    added = jnp.dot(
        jnp.concatenate([high, low, high], 1), three_ref[...], preferred_element_type=jnp.float32
    )
    out_ref[...] = field_ref[...] + added.reshape(field_ref.shape)


def box_kernel(
    bits, chunks, norm, weights_ref, cut_x_ref, cut_y_ref, index_ref, field_ref, table_ref, base_ref,
    turn_ref, host_ref, mix_ref, out_ref, edge_ref, part_ref, full_ref, *scratch
):
    got, kept = scratch[:bits], scratch[bits : 2 * bits]
    send_sem, recv_sem, out_sem = scratch[2 * bits :]
    _, group, row_count, ny = field_ref.shape
    span, kbox = host_ref.shape[-2:]
    owned, khalf, levels = span // group, kbox // 2, cut_x_ref.shape[0]
    half = owned // 2
    now = pl.program_id(0)
    me = lax.axis_index("row")
    member = lax.axis_index("member")
    mine = [(me // (1 << b)) % 2 for b in range(bits)]
    peer = [me + (1 << b) * (1 - 2 * mine[b]) for b in range(bits)]
    barrier = pltpu.get_barrier_semaphore()

    @pl.when(now == 0)
    def _():
        for b in range(bits):
            pl.semaphore_signal(barrier, inc=1, device_id=(member, peer[b]), device_id_type=MESH)
        edge = cut_x_ref[0]
        for level in range(levels):
            edge = jnp.maximum(edge, jnp.maximum(cut_x_ref[level], cut_y_ref[level]))
        edge_ref[0] = edge

    def lead(step, bit_value):
        return (slice(None),) * (bits - 1 - step) + (bit_value,)

    def remote(source, target, stage, chunk, bit):
        return pltpu.make_async_remote_copy(
            src_ref=source,
            dst_ref=target,
            send_sem=send_sem.at[chunk, stage],
            recv_sem=recv_sem.at[chunk, stage],
            device_id=(member, peer[bit]),
            device_id_type=MESH,
        )

    def held(step):
        return part_ref if step == 0 else kept[step - 1]

    def reduce_copy(step, chunk):
        source = held(step).at[(chunk,) + lead(step, 1 - mine[step])]
        return remote(source, got[step].at[chunk], step, chunk, step)

    def gather_copy(step, chunk):
        fixed = tuple(mine[b] for b in range(step, -1, -1))
        block = full_ref.at[(chunk,) + (slice(None),) * (bits - 1 - step) + fixed]
        return remote(block, block, bits + step, chunk, step)

    def out_copy(chunk):
        return pltpu.make_async_copy(full_ref.at[chunk], out_ref.at[chunk], out_sem.at[chunk])

    slot = lax.broadcasted_iota(jnp.int32, (span, kbox), 0)
    column = lax.broadcasted_iota(jnp.int32, (span, kbox), 1)
    line = slot % owned < half

    def swap(values):
        return jnp.where(
            line, pltpu.roll(values, span - half, 0), pltpu.roll(values, half, 0)
        )

    def mixed(values, axis):
        total = 0.0
        for _ in range(3):
            piece = values.astype(jnp.bfloat16)
            values = values - piece.astype(jnp.float32)
            total = total + lax.dot_general(
                piece,
                mix_ref[...],
                (((1,), (axis,)), ((), ())),
                preferred_element_type=jnp.float32,
            )
        return total

    def pull(chunk):
        both = mixed(kept[bits - 1][chunk] * norm, 0)
        even, odd = both[:, :kbox], both[:, kbox:]
        even_s, odd_s = swap(even), swap(odd)
        real = jnp.where(line, even - odd_s, even_s + odd)
        imag = jnp.where(line, -(odd + even_s), even - odd_s)
        wave = me * half + slot % half
        wave = jnp.where((wave == 0) & (slot % owned >= half), khalf, wave)
        steps = levels // group
        scale = jnp.zeros((span, kbox), jnp.float32)
        for k in range(group):
            level = (chunk % steps) * group + k
            inside = (jnp.abs(column - khalf) <= cut_x_ref[level]) & (wave <= cut_y_ref[level])
            blend = jnp.where(inside, weights_ref[index_ref[level], chunk // steps], 0.0)
            scale = jnp.where(slot // owned == k, blend, scale)
        real = scale * (host_ref[0, chunk] - real)
        imag = scale * (host_ref[1, chunk] - imag)
        real_s, imag_s = swap(real), swap(imag)
        cosine = jnp.where(line, real + real_s, imag - imag_s)
        sine = jnp.where(line, -(imag + imag_s), real - real_s)
        own = tuple(mine[b] for b in range(bits - 1, -1, -1))
        full_ref[(chunk,) + own] = mixed(jnp.concatenate([cosine, sine], 1), 1)

    def advance(stage, chunk):
        if stage < bits:
            reduce_copy(stage, chunk).wait()
            own = held(stage)[(chunk,) + lead(stage, mine[stage])]
            kept[stage][chunk] = own + got[stage][chunk]
            if stage + 1 < bits:
                reduce_copy(stage + 1, chunk).start()
            else:
                pull(chunk)
                gather_copy(bits - 1, chunk).start()
        else:
            step = 2 * bits - 1 - stage
            gather_copy(step, chunk).wait()
            if step > 0:
                gather_copy(step - 1, chunk).start()
            else:
                out_copy(chunk).start()

    @pl.when(now < chunks)
    def _():
        high, low = halves(field_ref[...].reshape(group * row_count, ny))
        both = jnp.dot(high, table_ref[...], preferred_element_type=jnp.float32)
        rest = jnp.dot(low, table_ref[:, :kbox], preferred_element_type=jnp.float32)
        part = both[:, :kbox] + both[:, kbox:] + rest
        x_high, x_low = halves(local_modes(base_ref, turn_ref))
        x_three = jnp.concatenate([x_high, x_high, x_low], 0)
        cube = (2,) * bits
        for k in range(group):
            high, low = halves(part[k * row_count : (k + 1) * row_count])
            moded = lax.dot_general(
                jnp.concatenate([high, low, high], 0),
                x_three,
                (((0,), (0,)), ((), ())),
                preferred_element_type=jnp.float32,
            )
            where = (now,) + (slice(None),) * bits + (slice(k * owned, (k + 1) * owned),)
            part_ref[where] = moded.reshape(cube + (owned, kbox))

    @pl.when(now == 0)
    def _():
        pl.semaphore_wait(barrier, bits)

    for stage in range(2 * bits - 1, -1, -1):
        chunk = now - 1 - stage

        @pl.when((chunk >= 0) & (chunk < chunks))
        def _(stage=stage, chunk=chunk):
            advance(stage, chunk)

    @pl.when(now < chunks)
    def _():
        reduce_copy(0, now).start()

    @pl.when(now == pl.num_programs(0) - 1)
    def _():
        for chunk in range(chunks):
            out_copy(chunk).wait()


def box_modes(scalars, field, table, base, turn, host, mix, group):
    variables, levels, row_count, ny = field.shape
    devices, kbox = turn.shape[0], host.shape[-1]
    chunks, span = host.shape[1:3]
    steps = levels // group
    bits = devices.bit_length() - 1
    cube = (2,) * bits
    sizes = [
        pltpu.VMEM((chunks,) + (2,) * (bits - 1 - step) + (span, kbox), jnp.float32)
        for step in range(bits)
    ]

    def chunk_at(now):
        chunk = jnp.minimum(now, chunks - 1)
        return (chunk // steps, chunk % steps, 0, 0)

    def whole(array):
        return pl.BlockSpec(array.shape, lambda now: (0,) * array.ndim)

    smem = pl.BlockSpec(memory_space=pltpu.SMEM)
    return pl.pallas_call(
        functools.partial(box_kernel, bits, chunks, 1.0 / (row_count * devices * ny)),
        grid=(chunks + 2 * bits,),
        out_shape=(
            jax.ShapeDtypeStruct((chunks,) + cube + (span, kbox), jnp.float32),
            jax.ShapeDtypeStruct((1,), jnp.int32),
        ),
        in_specs=[smem] * 4
        + [
            pl.BlockSpec((1, group, row_count, ny), chunk_at),
            whole(table),
            whole(base),
            pl.BlockSpec((1, 2, kbox), lambda now: (lax.axis_index("row"), 0, 0)),
            whole(host),
            whole(mix),
        ],
        out_specs=(pl.BlockSpec(memory_space=pl.ANY), smem),
        scratch_shapes=[pltpu.VMEM((chunks,) + cube + (span, kbox), jnp.float32)] * 2
        + sizes * 2
        + [
            pltpu.SemaphoreType.DMA((chunks, 2 * bits)),
            pltpu.SemaphoreType.DMA((chunks, 2 * bits)),
            pltpu.SemaphoreType.DMA((chunks,)),
        ],
        compiler_params=pltpu.CompilerParams(
            collective_id=0, has_side_effects=True, vmem_limit_bytes=48 * 1024 * 1024
        ),
    )(*scalars, field, table, base, turn, host, mix)


def nudge(field, host, weights, cut_x, cut_y, table_index):
    variables, levels, row_count, ny = field.shape
    owned, kbox = host.shape[0], host.shape[-1]
    khalf, half = kbox // 2, owned // 2
    devices = lax.axis_size("row")
    nx = row_count * devices
    fields = variables * levels

    column = np.arange(kbox)
    y_wave = column // owned * half + column % half
    y_sine = column % owned >= half
    y_high, y_low = np_halves(real_modes(ny, ny, y_wave, y_sine))
    table_y = jnp.asarray(np.concatenate([y_high, y_low], 1))
    table_back = jnp.asarray(np.concatenate([y_high.T, y_low.T], 0))
    x_wave, x_sine = column % khalf, column >= khalf
    start = np.arange(devices) * row_count
    base = np.concatenate(
        [real_modes(row_count, nx, x_wave, column < 0), real_modes(row_count, nx, x_wave, column >= 0)]
    )
    turn_cos = real_modes(start, nx, x_wave, column < 0)
    turn_sin = real_modes(start, nx, x_wave, column >= 0)
    turn = np.stack(
        [np.where(x_sine, turn_sin, turn_cos), np.where(x_sine, turn_cos, -turn_sin)], 1
    )
    base = jnp.asarray(base.astype(np.float32))
    turn = jnp.asarray(turn.astype(np.float32))
    wave = column - khalf
    inside = np.abs(wave) < khalf
    mc = ((column[:, None] == np.abs(wave)[None, :]) & inside).astype(np.float32)
    ms = ((column[:, None] == np.abs(wave)[None, :] + khalf) & inside) * np.sign(wave)
    ms = ms.astype(np.float32)

    group = math.gcd(levels, 3)
    steps = levels // group
    grid_block = pl.BlockSpec((1, group, row_count, ny), lambda v, g: (v, g, 0, 0))
    span = group * owned
    mode_block = pl.BlockSpec(
        (1, devices, span, kbox), lambda v, g: (v * steps + g, 0, 0, 0)
    )

    def whole(*shape):
        return pl.BlockSpec(shape, lambda v, g: (0,) * len(shape))

    local_turn = pl.BlockSpec((1, 2, kbox), lambda v, g: (lax.axis_index("row"), 0, 0))
    params = pltpu.CompilerParams(vmem_limit_bytes=48 * 1024 * 1024)
    placed = host.reshape(half, 2, 2, fields, kbox).transpose(2, 3, 1, 0, 4)
    modes, edge = box_modes(
        (weights, cut_x, cut_y, table_index),
        field,
        table_y,
        base,
        turn,
        placed.reshape(2, fields // group, span, kbox),
        jnp.asarray(np.concatenate([mc, ms], 1)).astype(jnp.bfloat16),
        group,
    )
    modes = modes.reshape(fields // group, devices, span, kbox)

    inverse = pl.pallas_call(
        inverse_kernel,
        grid=(variables, steps),
        out_shape=jax.ShapeDtypeStruct(field.shape, jnp.float32),
        in_specs=[grid_block, mode_block, whole(2 * kbox, ny), whole(2 * row_count, kbox), local_turn],
        out_specs=grid_block,
        scratch_shapes=[pltpu.VMEM((3 * kbox, ny), jnp.bfloat16)],
        compiler_params=params,
    )
    return lax.cond(
        edge[0] >= khalf,
        lambda *args: general(*args[:6]),
        lambda *args: inverse(args[0], *args[6:]),
        field, host, weights, cut_x, cut_y, table_index, modes, table_back, base, turn,
    )


def solution(mesh):
    return jax.shard_map(
        nudge,
        mesh=mesh,
        in_specs=(
            P("member", None, "row", None),
            P("row", None, "member", None, None),
            P(),
            P(),
            P(),
            P(),
        ),
        out_specs=P("member", None, "row", None),
        check_vma=False,
    )
```

```python
import functools
import math

import jax
import jax.numpy as jnp
import numpy as np
from jax import lax
from jax.experimental import pallas as pl
from jax.experimental.pallas import tpu as pltpu
from jax.sharding import PartitionSpec as P

TABLE = 8
MESH = pl.DeviceIdType.MESH
VMEM_BYTES = 63_000_000
HIGHEST = lax.Precision.HIGHEST


def box_wave(index, khalf):
    half = index // 2
    return jnp.where(index % 2 == 0, half, jnp.where(index == 1, -khalf, -half))


def wave_tables(positions, length, waves):
    phase = jnp.mod(positions[:, None] * waves[None, :], length).astype(jnp.float32) * (
        2.0 * math.pi / length
    )
    return (jnp.cos(phase), jnp.sin(phase))


def general(field, host, weights, cut_x, cut_y, table_index):
    variables, levels, row_count, ny = field.shape
    owned, kbox = host.shape[0], host.shape[-1]
    fields = variables * levels
    devices = lax.axis_size("row")
    nx = row_count * devices
    place = lax.axis_index("row")
    local_rows = place * row_count + lax.iota(jnp.int32, row_count)
    x_waves = lax.iota(jnp.int32, kbox) - kbox // 2
    y_waves = box_wave(lax.iota(jnp.int32, kbox), kbox // 2)
    own_waves = box_wave(place * owned + lax.iota(jnp.int32, owned), kbox // 2)
    onehot = (table_index[:, None] == lax.iota(jnp.int32, TABLE)[None, :]).astype(jnp.float32)
    blend = jnp.dot(onehot, weights, precision=HIGHEST)
    mask_x = (jnp.abs(x_waves)[None, :] <= cut_x[:, None]).astype(jnp.float32)
    mask_y = (jnp.abs(own_waves)[None, :] <= cut_y[:, None]).astype(jnp.float32)
    scale = blend.T[:, :, None, None] * mask_y[None, :, :, None] * mask_x[None, :, None, :]
    cos_y, sin_y = wave_tables(lax.iota(jnp.int32, ny), ny, y_waves)
    cos_x, sin_x = wave_tables(local_rows, nx, x_waves)
    table_y = jnp.concatenate([cos_y, -sin_y], 1)
    table_x = jnp.stack([jnp.concatenate([cos_x, -sin_x], 1), jnp.concatenate([sin_x, cos_x], 1)])

    def one(pair):
        grid, wanted, factor = pair
        spread = jnp.dot(grid, table_y, precision=HIGHEST).reshape(row_count, 2, kbox)
        parts = jnp.einsum("xck,cxq->kq", spread, table_x, precision=HIGHEST)
        parts = parts.reshape(devices, owned, 2, kbox)
        moved = lax.all_to_all(parts, "row", split_axis=0, concat_axis=0, tiled=True)
        spectrum = jnp.sum(moved, 0) / (nx * ny)
        delta = factor[:, None, :] * (wanted - spectrum)
        box = lax.all_gather(delta, "row", axis=0, tiled=True).reshape(kbox, 2 * kbox)
        back = jnp.einsum("kq,cxq->xck", box, table_x, precision=HIGHEST)
        return grid + jnp.dot(back.reshape(row_count, 2 * kbox), table_y.T, precision=HIGHEST)

    wanted = host.transpose(2, 3, 0, 1, 4).reshape(fields, owned, 2, kbox)
    result = lax.map(
        one, (field.reshape(fields, row_count, ny), wanted, scale.reshape(fields, owned, kbox))
    )
    return result.reshape(field.shape)


def halves(values):
    high = values.astype(jnp.bfloat16)
    return high, (values - high.astype(jnp.float32)).astype(jnp.bfloat16)


def np_halves(values):
    values = values.astype(np.float32)
    high = values.astype(jnp.bfloat16)
    return high, (values - high.astype(np.float32)).astype(jnp.bfloat16)


def real_modes(positions, length, waves, is_sine):
    if isinstance(positions, int):
        positions = np.arange(positions)
    phase = (positions[:, None] * waves[None, :]) % length * (2.0 * np.pi / length)
    return np.where(is_sine[None, :], np.sin(phase), np.cos(phase))


def local_modes(base_ref, turn_ref):
    count = base_ref.shape[0] // 2
    return base_ref[:count] * turn_ref[0, :1] + base_ref[count:] * turn_ref[0, 1:2]


def inverse_kernel(field_ref, modes_ref, table_ref, base_ref, turn_ref, out_ref, three_ref):
    _, count, row_count, ny = field_ref.shape
    kbox = base_ref.shape[1]
    owned = modes_ref.shape[2] // count
    x_high, x_low = halves(local_modes(base_ref, turn_ref))
    x_three = jnp.concatenate([x_high, x_high, x_low], 1)

    @pl.when((pl.program_id(0) == 0) & (pl.program_id(1) == 0))
    def _():
        three_ref[:kbox] = table_ref[:kbox]
        three_ref[kbox:] = table_ref[...]

    parts = []
    for k in range(count):
        high, low = halves(modes_ref[0, :, k * owned : (k + 1) * owned].reshape(kbox, kbox))
        parts.append(
            lax.dot_general(
                x_three,
                jnp.concatenate([high, low, high], 1),
                (((1,), (1,)), ((), ())),
                preferred_element_type=jnp.float32,
            )
        )
    high, low = halves(jnp.concatenate(parts, 0))
    added = jnp.dot(
        jnp.concatenate([high, low, high], 1), three_ref[...], preferred_element_type=jnp.float32
    )
    out_ref[...] = field_ref[...] + added.reshape(field_ref.shape)


def stage_step(stage):
    return 2 * stage + 1


def box_kernel(
    bits, chunks, norm, weights_ref, cut_x_ref, cut_y_ref, index_ref, field_ref, table_ref, base_ref,
    turn_ref, host_ref, mix_ref, out_ref, edge_ref, part_ref, full_ref, *scratch
):
    got, kept = scratch[:bits], scratch[bits : 2 * bits]
    send_sem, recv_sem, out_sem = scratch[2 * bits :]
    _, group, row_count, ny = field_ref.shape
    span, kbox = host_ref.shape[-2:]
    owned, khalf, levels = span // group, kbox // 2, cut_x_ref.shape[0]
    half = owned // 2
    now = pl.program_id(0)
    me = lax.axis_index("row")
    member = lax.axis_index("member")
    mine = [(me // (1 << b)) % 2 for b in range(bits)]
    peer = [me + (1 << b) * (1 - 2 * mine[b]) for b in range(bits)]
    barrier = pltpu.get_barrier_semaphore()

    @pl.when(now == 0)
    def _():
        for b in range(bits):
            pl.semaphore_signal(barrier, inc=1, device_id=(member, peer[b]), device_id_type=MESH)
        edge = cut_x_ref[0]
        for level in range(levels):
            edge = jnp.maximum(edge, jnp.maximum(cut_x_ref[level], cut_y_ref[level]))
        edge_ref[0] = edge

    def lead(step, bit_value):
        return (slice(None),) * (bits - 1 - step) + (bit_value,)

    def remote(source, target, stage, chunk, bit):
        return pltpu.make_async_remote_copy(
            src_ref=source,
            dst_ref=target,
            send_sem=send_sem.at[chunk, stage],
            recv_sem=recv_sem.at[chunk, stage],
            device_id=(member, peer[bit]),
            device_id_type=MESH,
        )

    def held(step):
        return part_ref if step == 0 else kept[step - 1]

    def reduce_copy(step, chunk):
        source = held(step).at[(chunk,) + lead(step, 1 - mine[step])]
        return remote(source, got[step].at[chunk], step, chunk, step)

    def gather_copy(step, chunk):
        fixed = tuple(mine[b] for b in range(step, -1, -1))
        block = full_ref.at[(chunk,) + (slice(None),) * (bits - 1 - step) + fixed]
        return remote(block, block, bits + step, chunk, step)

    def out_copy(chunk):
        return pltpu.make_async_copy(full_ref.at[chunk], out_ref.at[chunk], out_sem.at[chunk])

    slot = lax.broadcasted_iota(jnp.int32, (span, kbox), 0)
    column = lax.broadcasted_iota(jnp.int32, (span, kbox), 1)
    line = slot % owned < half

    def swap(values):
        return jnp.where(
            line, pltpu.roll(values, span - half, 0), pltpu.roll(values, half, 0)
        )

    def mixed(values, axis):
        total = 0.0
        for _ in range(3):
            piece = values.astype(jnp.bfloat16)
            values = values - piece.astype(jnp.float32)
            total = total + lax.dot_general(
                piece,
                mix_ref[...],
                (((1,), (axis,)), ((), ())),
                preferred_element_type=jnp.float32,
            )
        return total

    def pull(chunk):
        both = mixed(kept[bits - 1][chunk] * norm, 0)
        even, odd = both[:, :kbox], both[:, kbox:]
        even_s, odd_s = swap(even), swap(odd)
        real = jnp.where(line, even - odd_s, even_s + odd)
        imag = jnp.where(line, -(odd + even_s), even - odd_s)
        wave = me * half + slot % half
        wave = jnp.where((wave == 0) & (slot % owned >= half), khalf, wave)
        steps = levels // group
        scale = jnp.zeros((span, kbox), jnp.float32)
        for k in range(group):
            level = (chunk % steps) * group + k
            inside = (jnp.abs(column - khalf) <= cut_x_ref[level]) & (wave <= cut_y_ref[level])
            blend = jnp.where(inside, weights_ref[chunk // steps, index_ref[level]], 0.0)
            scale = jnp.where(slot // owned == k, blend, scale)
        real = scale * (host_ref[0, chunk] - real)
        imag = scale * (host_ref[1, chunk] - imag)
        real_s, imag_s = swap(real), swap(imag)
        cosine = jnp.where(line, real + real_s, imag - imag_s)
        sine = jnp.where(line, -(imag + imag_s), real - real_s)
        own = tuple(mine[b] for b in range(bits - 1, -1, -1))
        full_ref[(chunk,) + own] = mixed(jnp.concatenate([cosine, sine], 1), 1)

    def advance(stage, chunk):
        if stage < bits:
            reduce_copy(stage, chunk).wait()
            own = held(stage)[(chunk,) + lead(stage, mine[stage])]
            kept[stage][chunk] = own + got[stage][chunk]
            if stage + 1 < bits:
                reduce_copy(stage + 1, chunk).start()
            else:
                pull(chunk)
                gather_copy(bits - 1, chunk).start()
        else:
            step = 2 * bits - 1 - stage
            gather_copy(step, chunk).wait()
            if step > 0:
                gather_copy(step - 1, chunk).start()
            else:
                out_copy(chunk).start()

    @pl.when(now < chunks)
    def _():
        high, low = halves(field_ref[...].reshape(group * row_count, ny))
        both = jnp.dot(high, table_ref[...], preferred_element_type=jnp.float32)
        rest = jnp.dot(low, table_ref[:, :kbox], preferred_element_type=jnp.float32)
        part = both[:, :kbox] + both[:, kbox:] + rest
        x_high, x_low = halves(local_modes(base_ref, turn_ref))
        x_three = jnp.concatenate([x_high, x_high, x_low], 0)
        cube = (2,) * bits
        for k in range(group):
            high, low = halves(part[k * row_count : (k + 1) * row_count])
            moded = lax.dot_general(
                jnp.concatenate([high, low, high], 0),
                x_three,
                (((0,), (0,)), ((), ())),
                preferred_element_type=jnp.float32,
            )
            where = (now,) + (slice(None),) * bits + (slice(k * owned, (k + 1) * owned),)
            part_ref[where] = moded.reshape(cube + (owned, kbox))

    @pl.when(now == 0)
    def _():
        pl.semaphore_wait(barrier, bits)

    for stage in range(2 * bits):
        chunk = now - stage_step(stage)

        @pl.when((chunk >= 0) & (chunk < chunks))
        def _(stage=stage, chunk=chunk):
            advance(stage, chunk)

    @pl.when(now < chunks)
    def _():
        reduce_copy(0, now).start()

    @pl.when(now == pl.num_programs(0) - 1)
    def _():
        for chunk in range(chunks):
            out_copy(chunk).wait()


def box_modes(scalars, field, table, base, turn, host, mix, group):
    variables, levels, row_count, ny = field.shape
    devices, kbox = turn.shape[0], host.shape[-1]
    chunks, span = host.shape[1:3]
    steps = levels // group
    bits = devices.bit_length() - 1
    cube = (2,) * bits
    sizes = [
        pltpu.VMEM((chunks,) + (2,) * (bits - 1 - step) + (span, kbox), jnp.float32)
        for step in range(bits)
    ]

    def chunk_at(now):
        chunk = jnp.minimum(now, chunks - 1)
        return (chunk // steps, chunk % steps, 0, 0)

    def whole(array):
        return pl.BlockSpec(array.shape, lambda now: (0,) * array.ndim)

    smem = pl.BlockSpec(memory_space=pltpu.SMEM)
    return pl.pallas_call(
        functools.partial(box_kernel, bits, chunks, 1.0 / (row_count * devices * ny)),
        grid=(chunks + stage_step(2 * bits - 1),),
        out_shape=(
            jax.ShapeDtypeStruct((chunks,) + cube + (span, kbox), jnp.float32),
            jax.ShapeDtypeStruct((1,), jnp.int32),
        ),
        in_specs=[smem] * 4
        + [
            pl.BlockSpec((1, group, row_count, ny), chunk_at),
            whole(table),
            whole(base),
            pl.BlockSpec((1, 2, kbox), lambda now: (lax.axis_index("row"), 0, 0)),
            whole(host),
            whole(mix),
        ],
        out_specs=(pl.BlockSpec(memory_space=pl.ANY), smem),
        scratch_shapes=[pltpu.VMEM((chunks,) + cube + (span, kbox), jnp.float32)] * 2
        + sizes * 2
        + [
            pltpu.SemaphoreType.DMA((chunks, 2 * bits)),
            pltpu.SemaphoreType.DMA((chunks, 2 * bits)),
            pltpu.SemaphoreType.DMA((chunks,)),
        ],
        compiler_params=pltpu.CompilerParams(
            collective_id=0, has_side_effects=True, vmem_limit_bytes=VMEM_BYTES
        ),
    )(*scalars, field, table, base, turn, host, mix)


def nudge(field, host, weights, cut_x, cut_y, table_index):
    variables, levels, row_count, ny = field.shape
    owned, kbox = host.shape[0], host.shape[-1]
    khalf, half = kbox // 2, owned // 2
    devices = lax.axis_size("row")
    nx = row_count * devices
    fields = variables * levels

    column = np.arange(kbox)
    y_wave = column // owned * half + column % half
    y_sine = column % owned >= half
    y_high, y_low = np_halves(real_modes(ny, ny, y_wave, y_sine))
    table_y = jnp.asarray(np.concatenate([y_high, y_low], 1))
    table_back = jnp.asarray(np.concatenate([y_high.T, y_low.T], 0))
    x_wave, x_sine = column % khalf, column >= khalf
    start = np.arange(devices) * row_count
    base = np.concatenate(
        [real_modes(row_count, nx, x_wave, column < 0), real_modes(row_count, nx, x_wave, column >= 0)]
    )
    turn_cos = real_modes(start, nx, x_wave, column < 0)
    turn_sin = real_modes(start, nx, x_wave, column >= 0)
    turn = np.stack(
        [np.where(x_sine, turn_sin, turn_cos), np.where(x_sine, turn_cos, -turn_sin)], 1
    )
    base = jnp.asarray(base.astype(np.float32))
    turn = jnp.asarray(turn.astype(np.float32))
    wave = column - khalf
    inside = np.abs(wave) < khalf
    mc = ((column[:, None] == np.abs(wave)[None, :]) & inside).astype(np.float32)
    ms = ((column[:, None] == np.abs(wave)[None, :] + khalf) & inside) * np.sign(wave)
    ms = ms.astype(np.float32)

    group = levels
    steps = levels // group
    grid_block = pl.BlockSpec((1, group, row_count, ny), lambda v, g: (v, g, 0, 0))
    span = group * owned
    mode_block = pl.BlockSpec(
        (1, devices, span, kbox), lambda v, g: (v * steps + g, 0, 0, 0)
    )

    def whole(*shape):
        return pl.BlockSpec(shape, lambda v, g: (0,) * len(shape))

    local_turn = pl.BlockSpec((1, 2, kbox), lambda v, g: (lax.axis_index("row"), 0, 0))
    params = pltpu.CompilerParams(vmem_limit_bytes=VMEM_BYTES)
    placed = host.reshape(half, 2, 2, fields, kbox).transpose(2, 3, 1, 0, 4)
    modes, edge = box_modes(
        (weights.T, cut_x, cut_y, table_index),
        field,
        table_y,
        base,
        turn,
        placed.reshape(2, fields // group, span, kbox),
        jnp.asarray(np.concatenate([mc, ms], 1)).astype(jnp.bfloat16),
        group,
    )
    modes = modes.reshape(fields // group, devices, span, kbox)

    inverse = pl.pallas_call(
        inverse_kernel,
        grid=(variables, steps),
        out_shape=jax.ShapeDtypeStruct(field.shape, jnp.float32),
        in_specs=[grid_block, mode_block, whole(2 * kbox, ny), whole(2 * row_count, kbox), local_turn],
        out_specs=grid_block,
        scratch_shapes=[pltpu.VMEM((3 * kbox, ny), jnp.bfloat16)],
        compiler_params=params,
    )
    return lax.cond(
        edge[0] >= khalf,
        lambda *args: general(*args[:6]),
        lambda *args: inverse(args[0], *args[6:]),
        field, host, weights, cut_x, cut_y, table_index, modes, table_back, base, turn,
    )


def solution(mesh):
    return jax.shard_map(
        nudge,
        mesh=mesh,
        in_specs=(
            P("member", None, "row", None),
            P("row", None, "member", None, None),
            P(),
            P(),
            P(),
            P(),
        ),
        out_specs=P("member", None, "row", None),
        check_vma=False,
    )
```
